32 devices in a mesh: batch: 4 (over z), rows: 8 (over y, x, core).
Axes of the slice: x: 2, y: 2, z: 4, core: 2. Of those that a mesh axis runs over, the one named last changes fastest.
Arguments:
- level_two: bfloat16 [8, 64, 256, 256], P('batch', 'rows'), parts along dimension 0, may hold values from -130 to 130
- level_three: bfloat16 [8, 32, 128, 512], P('batch', 'rows'), parts along dimension 0, may hold values from -130 to 130
- level_four: bfloat16 [8, 16, 64, 1024], P('batch', 'rows'), parts along dimension 0, may hold values from -130 to 130
- level_five: bfloat16 [8, 8, 32, 2048], P('batch', 'rows'), parts along dimension 0, may hold values from -130 to 130
- lateral_two: bfloat16 [256, 256], replicated, may hold values from -0.375 to 0.375
- lateral_three: bfloat16 [512, 256], replicated, may hold values from -0.25 to 0.25
- lateral_four: bfloat16 [1024, 256], replicated, may hold values from -0.1875 to 0.1875
- lateral_five: bfloat16 [2048, 256], replicated, may hold values from -0.125 to 0.125
- lateral_bias: float32 [4, 256], replicated, may hold values from -4 to 4
- smooth_weight: bfloat16 [4, 3, 768, 256], replicated, may hold values from -0.125 to 0.125
- norm_gain: float32 [4, 256], replicated, may hold values from 0.5 to 1.5
- norm_shift: float32 [4, 256], replicated, may hold values from -2 to 2
Outputs:
- pyramid_two: bfloat16 [8, 64, 256, 256], P('batch', 'rows'), parts along dimension 0
- pyramid_three: bfloat16 [8, 32, 128, 256], P('batch', 'rows'), parts along dimension 0
- pyramid_four: bfloat16 [8, 16, 64, 256], P('batch', 'rows'), parts along dimension 0
- pyramid_five: bfloat16 [8, 8, 32, 256], P('batch', 'rows'), parts along dimension 0
The draws below stay inside these ranges and needn't reach their ends.
There are 4 independent parts, one for each index of `batch`. The reference program is written for one: setup_inputs(seed, part) draws one part's arguments, and reference() takes and returns one part's arrays. A program takes and returns all parts, laid end to end along the dimension named above; an argument that names none is the same for every part. Nothing has to cross between parts.
All inputs are finite; a program needn't handle non-finite values.
Results may differ from the reference program's by a relative error of at most 0.0054.
Values may be sent and summed in bfloat16 or wider, within the bound.
A program may use at most 128 MiB of HBM per device.

```python
import math
import jax
import jax.numpy as jnp
from jax import lax

CHANNELS = 256
DEPTH_TWO = 256
DEPTH_THREE = 512
DEPTH_FOUR = 1024
DEPTH_FIVE = 2048
GROUPS = 32
LEVELS = 4
IMAGES = 2
COLUMNS = 256
HEIGHT = 64


def feature_draw(key, rows_all, cols_all, depth_all, salt_code):
    base_key = jax.random.fold_in(key, salt_code)
    subkeys = jax.random.split(base_key, 3)
    relative = (jnp.arange(rows_all, dtype=jnp.float32) + 0.5) / rows_all
    jitter = jnp.exp(jax.random.uniform(subkeys[0], (IMAGES, rows_all), jnp.float32, 0.0, math.log(3.3)))
    row_scale = jnp.exp(math.log(3.0) * relative)[None, :] * jitter
    chan_scale = jnp.exp(jax.random.uniform(subkeys[1], (depth_all,), jnp.float32, -0.5 * math.log(10.0), 0.5 * math.log(10.0)))
    shape_all = (IMAGES, rows_all, cols_all, depth_all)
    values = jnp.clip(jax.random.normal(subkeys[2], shape_all, jnp.float32), -4.0, 4.0)
    return (values * row_scale[:, :, None, None] * chan_scale).astype(jnp.bfloat16)


def draw_level_two(key, part):
    return feature_draw(key, HEIGHT, COLUMNS, DEPTH_TWO, 11)


def draw_level_three(key, part):
    return feature_draw(key, HEIGHT // 2, COLUMNS // 2, DEPTH_THREE, 12)


def draw_level_four(key, part):
    return feature_draw(key, HEIGHT // 4, COLUMNS // 4, DEPTH_FOUR, 13)


def draw_level_five(key, part):
    return feature_draw(key, HEIGHT // 8, COLUMNS // 8, DEPTH_FIVE, 14)


def bell_draw(rng, shape, width, bound, kind=jnp.bfloat16):
    values = jax.random.normal(rng, shape, jnp.float32) * width
    return jnp.minimum(jnp.maximum(values, -bound), bound).astype(kind)


def setup_inputs(seed: int = 0, part: int = 0) -> dict:
    key_of = jax.random.split(jax.random.key(seed), 13)
    own_keys = jax.random.split(jax.random.fold_in(key_of[12], part), 13)
    return {
        "level_two": draw_level_two(jax.random.fold_in(jax.random.fold_in(key_of[12], part), 71), part),
        "level_three": draw_level_three(jax.random.fold_in(jax.random.fold_in(key_of[12], part), 71), part),
        "level_four": draw_level_four(jax.random.fold_in(jax.random.fold_in(key_of[12], part), 71), part),
        "level_five": draw_level_five(jax.random.fold_in(jax.random.fold_in(key_of[12], part), 71), part),
        "lateral_two": bell_draw(key_of[4], (DEPTH_TWO, CHANNELS), DEPTH_TWO ** -0.5, 0.375),
        "lateral_three": bell_draw(key_of[5], (DEPTH_THREE, CHANNELS), DEPTH_THREE ** -0.5, 0.25),
        "lateral_four": bell_draw(key_of[6], (DEPTH_FOUR, CHANNELS), DEPTH_FOUR ** -0.5, 0.1875),
        "lateral_five": bell_draw(key_of[7], (DEPTH_FIVE, CHANNELS), DEPTH_FIVE ** -0.5, 0.125),
        "lateral_bias": bell_draw(key_of[8], (LEVELS, CHANNELS), 1.0, 4.0, jnp.float32),
        "smooth_weight": bell_draw(key_of[9], (LEVELS, 3, 3 * CHANNELS, CHANNELS), (9 * CHANNELS) ** -0.5, 0.125),
        "norm_gain": jnp.clip(1.0 + 0.1 * jax.random.normal(key_of[10], (LEVELS, CHANNELS), jnp.float32), 0.5, 1.5),
        "norm_shift": bell_draw(key_of[11], (LEVELS, CHANNELS), 0.5, 2.0, jnp.float32),
    }


epsilon = 1e-05

def refine(widened, axis_pos):
    length = widened.shape[axis_pos] - 2
    before = lax.slice_in_dim(widened, 0, length, axis=axis_pos)
    middle = lax.slice_in_dim(widened, 1, length + 1, axis=axis_pos)
    beyond = lax.slice_in_dim(widened, 2, length + 2, axis=axis_pos)
    even_rows = 0.25 * before + 0.75 * middle
    odd_rows = 0.75 * middle + 0.25 * beyond
    stacked = jnp.stack([even_rows, odd_rows], axis_pos + 1)
    new_shape = list(widened.shape)
    new_shape[axis_pos] = 2 * length
    return stacked.reshape(new_shape)

def edge_columns(values):
    return jnp.concatenate([values[:, :, :1], values, values[:, :, -1:]], 2)

def lateral(feature, weight, bias_row):
    flattened = feature.reshape(-1, feature.shape[-1])
    result = jnp.dot(flattened, weight, preferred_element_type=jnp.float32) + bias_row
    return result.reshape(feature.shape[:-1] + (weight.shape[1],))

def conv_three(widened, weight):
    padded = jnp.pad(widened, ((0, 0), (0, 0), (1, 1), (0, 0)))
    strip_rows = widened.shape[1] - 2
    width_cells = widened.shape[2]
    channels = widened.shape[3]
    result = jnp.zeros((widened.shape[0] * strip_rows * width_cells, weight.shape[2]), jnp.float32)
    for tap_row in range(3):
        band_rows = padded[:, tap_row:tap_row + strip_rows]
        stacked = jnp.concatenate([band_rows[:, :, 0:width_cells], band_rows[:, :, 1:width_cells + 1], band_rows[:, :, 2:width_cells + 2]], 3)
        result = result + jnp.dot(stacked.reshape(-1, 3 * channels), weight[tap_row], preferred_element_type=jnp.float32)
    return result.reshape(widened.shape[0], strip_rows, width_cells, weight.shape[2])

def group_sums(conv_out):
    dims_all = conv_out.shape
    grouped = conv_out.reshape(dims_all[0], -1, GROUPS, dims_all[3] // GROUPS)
    return (lax.optimization_barrier(jnp.sum(grouped, axis=(1, 3))), lax.optimization_barrier(jnp.sum(grouped * grouped, axis=(1, 3))))

def normalize(conv_out, totals, squares, entries, gain_row, shift_row):
    mean_val = totals / entries
    variance = squares / entries - mean_val * mean_val
    scale_inv = lax.rsqrt(variance + epsilon)
    dims_all = conv_out.shape
    grouped = conv_out.reshape(dims_all[0], dims_all[1], dims_all[2], GROUPS, dims_all[3] // GROUPS)
    centred = (grouped - mean_val[:, None, None, :, None]) * scale_inv[:, None, None, :, None]
    return (centred.reshape(dims_all) * gain_row + shift_row).astype(jnp.bfloat16)

def reference(level_two, level_three, level_four, level_five, lateral_two, lateral_three, lateral_four, lateral_five, lateral_bias, smooth_weight, norm_gain, norm_shift):
    features = (level_two, level_three, level_four, level_five)
    weights = (lateral_two, lateral_three, lateral_four, lateral_five)
    laterals = [lateral(features[level_idx], weights[level_idx], lateral_bias[level_idx]) for level_idx in range(4)]
    merged_maps = [None, None, None, None]
    merged_maps[3] = laterals[3].astype(jnp.bfloat16)
    for level_idx in (2, 1, 0):
        coarse = merged_maps[level_idx + 1].astype(jnp.float32)
        widened = jnp.concatenate([coarse[:, :1], coarse, coarse[:, -1:]], 1)
        upsampled = refine(edge_columns(refine(widened, 1)), 2)
        merged_maps[level_idx] = (laterals[level_idx] + upsampled).astype(jnp.bfloat16)
    outputs = []
    for level_idx in range(4):
        widened = jnp.pad(merged_maps[level_idx], ((0, 0), (1, 1), (0, 0), (0, 0)))
        conv_out = conv_three(widened, smooth_weight[level_idx])
        totals, squares = group_sums(conv_out)
        entries = float(conv_out.shape[1] * conv_out.shape[2] * (conv_out.shape[3] // GROUPS))
        outputs.append(normalize(conv_out, totals, squares, entries, norm_gain[level_idx], norm_shift[level_idx]))
    return (outputs[0], outputs[1], outputs[2], outputs[3])
```

```python
import functools

import jax
import jax.numpy as jnp
from jax import lax
from jax.experimental import pallas as pl
from jax.experimental.pallas import tpu as pltpu
from jax.sharding import PartitionSpec as P

GROUPS = 32
EPSILON = 1e-05
F32 = jnp.float32
BF16 = jnp.bfloat16
MESH = pl.DeviceIdType.MESH


def bilinear(cols):
    half = cols // 2
    fine = lax.broadcasted_iota(jnp.int32, (cols, cols), 0)
    coarse = lax.broadcasted_iota(jnp.int32, (cols, cols), 1)
    second = coarse >= half
    coarse = jnp.where(second, coarse - half, coarse)
    near = fine // 2
    odd = fine % 2 == 1
    far = jnp.where(odd, jnp.minimum(near + 1, half - 1), jnp.maximum(near - 1, 0))
    value = jnp.where(coarse == near, 0.75, 0.0) + jnp.where(coarse == far, 0.25, 0.0)
    even_rows = value * jnp.where(second, 0.75, 0.25)
    odd_rows = value * jnp.where(second, 0.25, 0.75)
    return even_rows.astype(BF16), odd_rows.astype(BF16)


def mm(a, b):
    return jnp.dot(a, b, preferred_element_type=F32)


def kernel(n, geom, *refs):
    images, chans = geom["images"], geom["chans"]
    rows, cols = geom["rows"], geom["cols"]
    it = iter(refs)
    take = lambda count: [next(it) for _ in range(count)]
    feat_hbm, lat_hbm = take(4), take(4)
    bias, smooth_hbm, gain, shift = take(4)
    out_hbm = take(4)
    feat, lat_w = take(4), take(4)
    (smooth,) = take(1)
    big, conv, staged, sends, recvs = take(4), take(4), take(4), take(4), take(4)
    lats = [None] + take(3)
    ups = take(3)
    stat_two, stat_rest, got_two, got_rest = take(4)
    in_sem, w_sem, s_sem, out_sem = take(4)
    halo_send, halo_recv, two_send, two_recv, rest_send, rest_recv = take(6)

    me = lax.axis_index("rows")
    first, last = me == 0, me == n - 1

    feat_copy = [pltpu.make_async_copy(feat_hbm[k], feat[k], in_sem.at[k]) for k in range(4)]
    lat_copy = [pltpu.make_async_copy(lat_hbm[k], lat_w[k], w_sem.at[k]) for k in range(4)]
    smooth_copy = [
        pltpu.make_async_copy(smooth_hbm.at[k], smooth.at[k], s_sem.at[k]) for k in range(4)
    ]
    for k in (3, 2, 1, 0):
        lat_copy[k].start()
        feat_copy[k].start()
    for k in (3, 2, 0, 1):
        smooth_copy[k].start()

    barrier = pltpu.get_barrier_semaphore()
    for d in range(1, n):
        pl.semaphore_signal(
            barrier, inc=1, device_id={"rows": lax.rem(me + d, n)}, device_id_type=MESH
        )

    @pl.when(first)
    def _():
        for k in range(4):
            recvs[k][0] = jnp.zeros_like(recvs[k][0])

    @pl.when(last)
    def _():
        for k in range(4):
            recvs[k][1] = jnp.zeros_like(recvs[k][1])

    for k in range(3):
        even, odd = bilinear(cols[k])
        ups[k][0] = even
        ups[k][1] = odd

    def halo_copy(k, way):
        return pltpu.make_async_remote_copy(
            src_ref=sends[k].at[way],
            dst_ref=recvs[k].at[1 - way],
            send_sem=halo_send.at[k, way],
            recv_sem=halo_recv.at[k, 1 - way],
            device_id={"rows": lax.rem(me + (1 if way else n - 1), n)},
            device_id_type=MESH,
        )

    def halo_start(k):
        @pl.when(jnp.logical_not(first))
        def _():
            halo_copy(k, 0).start()

        @pl.when(jnp.logical_not(last))
        def _():
            halo_copy(k, 1).start()

    def halo_wait(k):
        @pl.when(jnp.logical_not(last))
        def _():
            halo_copy(k, 0).wait_recv()

        @pl.when(jnp.logical_not(first))
        def _():
            halo_copy(k, 1).wait_recv()

    def sent_wait(k):
        @pl.when(jnp.logical_not(first))
        def _():
            halo_copy(k, 0).wait_send()

        @pl.when(jnp.logical_not(last))
        def _():
            halo_copy(k, 1).wait_send()

    for k in (3, 2, 1):
        lat_copy[k].wait()
        feat_copy[k].wait()
        for i in range(images):
            flat = feat[k][i].reshape(rows[k] * cols[k], feat[k].shape[-1])
            value = mm(flat, lat_w[k][...]) + bias[k : k + 1, :]
            lats[k][i] = value.reshape(rows[k], cols[k], chans)
            sends[k][0, i] = value[: cols[k]].astype(BF16)
            sends[k][1, i] = value[(rows[k] - 1) * cols[k] :].astype(BF16)
        if k == 3:
            pl.semaphore_wait(barrier, n - 1)
        halo_start(k)
    lat_copy[0].wait()
    feat_copy[0].wait()
    for i in range(images):
        for way, y in ((0, 0), (1, rows[0] - 1)):
            sends[0][way, i] = (mm(feat[0][i, y], lat_w[0][...]) + bias[0:1, :]).astype(BF16)
    halo_start(0)

    def put(k, i, r, value):
        width = cols[k]
        spot = lax.broadcasted_iota(jnp.int32, value.shape, 0)
        before = jnp.where(spot == 0, 0.0, pltpu.roll(value, 1, 0))
        beyond = jnp.where(spot == width - 1, 0.0, pltpu.roll(value, width - 1, 0))
        big[k][i, r, :, 0:chans] = before.astype(BF16)
        big[k][i, r, :, chans : 2 * chans] = value.astype(BF16)
        big[k][i, r, :, 2 * chans :] = beyond.astype(BF16)

    def center(k, i, r):
        return big[k][i, r, :, chans : 2 * chans].astype(F32)

    def doubled(k, i, phase, r):
        pair = big[k + 1][i, pl.ds(r, 2), :, chans : 2 * chans]
        return mm(ups[k][phase], pair.reshape(cols[k], chans))

    for i in range(images):
        for y in range(rows[3]):
            put(3, i, y + 1, lats[3][i, y])
    halo_wait(3)
    for i in range(images):
        put(3, i, 0, jnp.where(first, center(3, i, 1), recvs[3][0, i].astype(F32)))
        put(3, i, rows[3] + 1, jnp.where(last, center(3, i, rows[3]), recvs[3][1, i].astype(F32)))

    def clear(k):
        @pl.when(first)
        def _():
            for i in range(images):
                big[k][i, 0] = jnp.zeros_like(big[k][i, 0])

        @pl.when(last)
        def _():
            for i in range(images):
                big[k][i, rows[k] + 1] = jnp.zeros_like(big[k][i, rows[k] + 1])

    def edges(k):
        for i in range(images):
            above = recvs[k][0, i].astype(F32) + doubled(k, i, 1, 0)
            below = recvs[k][1, i].astype(F32) + doubled(k, i, 0, rows[k] // 2)
            put(k, i, 0, jnp.where(first, center(k, i, 1), above))
            put(k, i, rows[k] + 1, jnp.where(last, center(k, i, rows[k]), below))

    for k in (2, 1):
        for i in range(images):
            for j in range(rows[k] // 2):
                put(k, i, 2 * j + 1, lats[k][i, 2 * j] + doubled(k, i, 0, j))
                put(k, i, 2 * j + 2, lats[k][i, 2 * j + 1] + doubled(k, i, 1, j + 1))
        halo_wait(k)
        edges(k)
        clear(k + 1)

    pairs = rows[0] // 2

    def merge_two(t, carry):
        i, j = t // pairs, t % pairs
        both = mm(feat[0][i, pl.ds(2 * j, 2)].reshape(2 * cols[0], -1), lat_w[0][...])
        both = both + bias[0:1, :]
        put(0, i, 2 * j + 1, both[: cols[0]] + doubled(0, i, 0, j))
        put(0, i, 2 * j + 2, both[cols[0] :] + doubled(0, i, 1, j + 1))
        return carry

    lax.fori_loop(0, images * pairs, merge_two, 0)

    def conv_rows(k, i, y, count):
        total = None
        for a in range(3):
            band = big[k][i, pl.ds(y + a, count)].reshape(count * cols[k], 3 * chans)
            part = mm(band, smooth[k, a])
            total = part if total is None else total + part
        conv[k][i, pl.ds(y, count)] = total.reshape(count, cols[k], chans)
        return jnp.sum(total, 0, keepdims=True), jnp.sum(total * total, 0, keepdims=True)

    stat_rest[...] = jnp.zeros_like(stat_rest)
    stat_two[...] = jnp.zeros_like(stat_two)

    def conv_whole(k):
        smooth_copy[k].wait()
        for i in range(images):
            total, square = conv_rows(k, i, 0, rows[k])
            slot = ((k - 1) * images + i) * 2
            stat_rest[slot : slot + 1, :] = total
            stat_rest[slot + 1 : slot + 2, :] = square

    conv_whole(3)
    conv_whole(2)

    smooth_copy[0].wait()
    inner = (rows[0] - 2) // 2
    for i in range(images):

        def conv_two(t, carry):
            total, square = conv_rows(0, i, 1 + 2 * t, 2)
            return carry[0] + total, carry[1] + square

        zero = jnp.zeros((1, chans), F32)
        total, square = lax.fori_loop(0, inner, conv_two, (zero, zero))
        stat_two[2 * i : 2 * i + 1, :] = total
        stat_two[2 * i + 1 : 2 * i + 2, :] = square
    halo_wait(0)
    edges(0)
    clear(0)
    clear(1)

    def conv_edges(t, carry):
        i, y = t // 2, (t % 2) * (rows[0] - 1)
        total, square = conv_rows(0, i, y, 1)
        stat_two[pl.ds(2 * i, 1), :] += total
        stat_two[pl.ds(2 * i + 1, 1), :] += square
        return carry

    lax.fori_loop(0, images * 2, conv_edges, 0)

    def stat_copies(mine, got, send_sem, recv_sem):
        return [
            pltpu.make_async_remote_copy(
                src_ref=mine,
                dst_ref=got.at[d],
                send_sem=send_sem.at[d],
                recv_sem=recv_sem.at[d],
                device_id={"rows": lax.rem(me + d, n)},
                device_id_type=MESH,
            )
            for d in range(1, n)
        ]

    two_copies = stat_copies(stat_two, got_two, two_send, two_recv)
    for copy in two_copies:
        copy.start()
    conv_whole(1)
    rest_copies = stat_copies(stat_rest, got_rest, rest_send, rest_recv)
    for copy in rest_copies:
        copy.start()

    size = chans // GROUPS
    same = lax.broadcasted_iota(jnp.int32, (chans, chans), 0) // size
    same = same == lax.broadcasted_iota(jnp.int32, (chans, chans), 1) // size
    same = jnp.where(same, 1.0, 0.0).astype(F32)

    def gathered(mine, got):
        total = mine[...]
        for d in range(1, n):
            total = total + got[d]
        return jnp.dot(
            total, same, precision=lax.Precision.HIGHEST, preferred_element_type=F32
        )

    def finish(k, i, total, square):
        entries = float(rows[k] * n * cols[k] * size)
        mean = total / entries
        variance = square / entries - mean * mean
        scale = lax.rsqrt(variance + EPSILON) * gain[k : k + 1, :]
        offset = shift[k : k + 1, :]

        def row(y, carry):
            staged[k][i, y] = ((conv[k][i, y] - mean) * scale + offset).astype(BF16)
            return carry

        lax.fori_loop(0, rows[k], row, 0)
        copy = pltpu.make_async_copy(staged[k].at[i], out_hbm[k].at[i], out_sem.at[k, i])
        copy.start()
        return copy

    out_copies = []
    for copy in two_copies:
        copy.wait_recv()
    sums = gathered(stat_two, got_two)
    for i in range(images):
        out_copies.append(
            finish(0, i, sums[2 * i : 2 * i + 1, :], sums[2 * i + 1 : 2 * i + 2, :])
        )
    for copy in rest_copies:
        copy.wait_recv()
    sums = gathered(stat_rest, got_rest)
    for k in (1, 2, 3):
        for i in range(images):
            slot = ((k - 1) * images + i) * 2
            out_copies.append(
                finish(k, i, sums[slot : slot + 1, :], sums[slot + 1 : slot + 2, :])
            )
    for k in range(4):
        sent_wait(k)
    for copy in two_copies + rest_copies:
        copy.wait_send()
    for copy in out_copies:
        copy.wait()


def per_device(n, *args):
    feats, lat_ws = args[0:4], args[4:8]
    bias, smooth, gain, shift = args[8:12]
    images, chans = feats[0].shape[0], lat_ws[0].shape[1]
    rows = [f.shape[1] for f in feats]
    cols = [f.shape[2] for f in feats]
    geom = {"images": images, "chans": chans, "rows": rows, "cols": cols}
    any_spec = pl.BlockSpec(memory_space=pl.ANY)
    vmem_spec = pl.BlockSpec(memory_space=pltpu.VMEM)
    outs = [jax.ShapeDtypeStruct((images, r, c, chans), BF16) for r, c in zip(rows, cols)]
    dma = pltpu.SemaphoreType.DMA
    rest_rows = -(-(3 * images * 2) // 8) * 8
    two_rows = -(-(images * 2) // 8) * 8
    scratch = (
        [pltpu.VMEM(f.shape, BF16) for f in feats]
        + [pltpu.VMEM(w.shape, BF16) for w in lat_ws]
        + [pltpu.VMEM(smooth.shape, BF16)]
        + [pltpu.VMEM((images, r + 2, c, 3 * chans), BF16) for r, c in zip(rows, cols)]
        + [pltpu.VMEM(o.shape, F32) for o in outs]
        + [pltpu.VMEM(o.shape, BF16) for o in outs]
        + [pltpu.VMEM((2, images, c, chans), BF16) for c in cols]
        + [pltpu.VMEM((2, images, c, chans), BF16) for c in cols]
        + [pltpu.VMEM(o.shape, F32) for o in outs[1:]]
        + [pltpu.VMEM((2, c, c), BF16) for c in cols[:3]]
        + [
            pltpu.VMEM((two_rows, chans), F32),
            pltpu.VMEM((rest_rows, chans), F32),
            pltpu.VMEM((n, two_rows, chans), F32),
            pltpu.VMEM((n, rest_rows, chans), F32),
        ]
        + [dma((4,)), dma((4,)), dma((4,)), dma((4, images))]
        + [dma((4, 2)), dma((4, 2)), dma((n,)), dma((n,)), dma((n,)), dma((n,))]
    )
    return pl.pallas_call(
        functools.partial(kernel, n, geom),
        out_shape=outs,
        in_specs=[any_spec] * 8 + [vmem_spec, any_spec, vmem_spec, vmem_spec],
        out_specs=[any_spec] * 4,
        scratch_shapes=scratch,
        compiler_params=pltpu.CompilerParams(
            collective_id=0, has_side_effects=True, vmem_limit_bytes=60 * 1024 * 1024
        ),
    )(*args)


def solution(mesh):
    strips = P("batch", "rows", None, None)
    run = functools.partial(per_device, mesh.shape["rows"])
    return jax.shard_map(
        lambda *args: tuple(run(*args)),
        mesh=mesh,
        in_specs=(strips,) * 4 + (P(),) * 8,
        out_specs=(strips,) * 4,
        check_vma=False,
    )
```

```python
import functools

import jax
import jax.numpy as jnp
from jax import lax
from jax.experimental import pallas as pl
from jax.experimental.pallas import tpu as pltpu
from jax.sharding import PartitionSpec as P

GROUPS = 32
EPSILON = 1e-05
F32 = jnp.float32
BF16 = jnp.bfloat16
MESH = pl.DeviceIdType.MESH
KERNEL_BYTES = 56 * 1024 * 1024


def bilinear(cols):
    half = cols // 2
    fine = lax.broadcasted_iota(jnp.int32, (cols, cols), 0)
    coarse = lax.broadcasted_iota(jnp.int32, (cols, cols), 1)
    second = coarse >= half
    coarse = jnp.where(second, coarse - half, coarse)
    near = fine // 2
    odd = fine % 2 == 1
    far = jnp.where(odd, jnp.minimum(near + 1, half - 1), jnp.maximum(near - 1, 0))
    value = jnp.where(coarse == near, 0.75, 0.0) + jnp.where(coarse == far, 0.25, 0.0)
    even_rows = value * jnp.where(second, 0.75, 0.25)
    odd_rows = value * jnp.where(second, 0.25, 0.75)
    return even_rows.astype(BF16), odd_rows.astype(BF16)


def mm(a, b):
    return jnp.dot(a, b, preferred_element_type=F32)


def kernel(n, geom, *refs):
    images, chans = geom["images"], geom["chans"]
    rows, cols = geom["rows"], geom["cols"]
    it = iter(refs)
    take = lambda count: [next(it) for _ in range(count)]
    feat_hbm, lat_hbm = take(4), take(4)
    bias, smooth_hbm = take(2)
    conv = take(4)
    sums_two, sums_rest = take(2)
    feat, lat_w = take(4), take(4)
    (smooth,) = take(1)
    big, sends, recvs = take(4), take(4), take(4)
    lats = [None] + take(3)
    ups = take(3)
    stat_two, stat_rest, got_two, got_rest = take(4)
    in_sem, w_sem, s_sem = take(3)
    halo_send, halo_recv, two_send, two_recv, rest_send, rest_recv = take(6)

    me = lax.axis_index("rows")
    first, last = me == 0, me == n - 1

    feat_copy = [pltpu.make_async_copy(feat_hbm[k], feat[k], in_sem.at[k]) for k in range(4)]
    lat_copy = [pltpu.make_async_copy(lat_hbm[k], lat_w[k], w_sem.at[k]) for k in range(4)]
    smooth_copy = [
        pltpu.make_async_copy(smooth_hbm.at[k], smooth.at[k], s_sem.at[k]) for k in range(4)
    ]
    for k in (3, 2, 1, 0):
        lat_copy[k].start()
        feat_copy[k].start()
    for k in (3, 2, 0, 1):
        smooth_copy[k].start()

    barrier = pltpu.get_barrier_semaphore()
    for d in range(1, n):
        pl.semaphore_signal(
            barrier, inc=1, device_id={"rows": lax.rem(me + d, n)}, device_id_type=MESH
        )

    @pl.when(first)
    def _():
        for k in range(4):
            recvs[k][0] = jnp.zeros_like(recvs[k][0])

    @pl.when(last)
    def _():
        for k in range(4):
            recvs[k][1] = jnp.zeros_like(recvs[k][1])

    for k in range(3):
        even, odd = bilinear(cols[k])
        ups[k][0] = even
        ups[k][1] = odd

    def halo_copy(k, way):
        return pltpu.make_async_remote_copy(
            src_ref=sends[k].at[way],
            dst_ref=recvs[k].at[1 - way],
            send_sem=halo_send.at[k, way],
            recv_sem=halo_recv.at[k, 1 - way],
            device_id={"rows": lax.rem(me + (1 if way else n - 1), n)},
            device_id_type=MESH,
        )

    def halo_start(k):
        @pl.when(jnp.logical_not(first))
        def _():
            halo_copy(k, 0).start()

        @pl.when(jnp.logical_not(last))
        def _():
            halo_copy(k, 1).start()

    def halo_wait(k):
        @pl.when(jnp.logical_not(last))
        def _():
            halo_copy(k, 0).wait_recv()

        @pl.when(jnp.logical_not(first))
        def _():
            halo_copy(k, 1).wait_recv()

    def sent_wait(k):
        @pl.when(jnp.logical_not(first))
        def _():
            halo_copy(k, 0).wait_send()

        @pl.when(jnp.logical_not(last))
        def _():
            halo_copy(k, 1).wait_send()

    for k in (3, 2, 1):
        lat_copy[k].wait()
        feat_copy[k].wait()
        for i in range(images):
            flat = feat[k][i].reshape(rows[k] * cols[k], feat[k].shape[-1])
            value = mm(flat, lat_w[k][...]) + bias[k : k + 1, :]
            lats[k][i] = value.reshape(rows[k], cols[k], chans)
            sends[k][0, i] = value[: cols[k]].astype(BF16)
            sends[k][1, i] = value[(rows[k] - 1) * cols[k] :].astype(BF16)
        if k == 3:
            pl.semaphore_wait(barrier, n - 1)
        halo_start(k)
    lat_copy[0].wait()
    feat_copy[0].wait()
    for i in range(images):
        for way, y in ((0, 0), (1, rows[0] - 1)):
            sends[0][way, i] = (mm(feat[0][i, y], lat_w[0][...]) + bias[0:1, :]).astype(BF16)
    halo_start(0)

    def put(k, i, r, value):
        width = cols[k]
        spot = lax.broadcasted_iota(jnp.int32, value.shape, 0)
        before = jnp.where(spot == 0, 0.0, pltpu.roll(value, 1, 0))
        beyond = jnp.where(spot == width - 1, 0.0, pltpu.roll(value, width - 1, 0))
        big[k][i, r, :, 0:chans] = before.astype(BF16)
        big[k][i, r, :, chans : 2 * chans] = value.astype(BF16)
        big[k][i, r, :, 2 * chans :] = beyond.astype(BF16)

    def center(k, i, r):
        return big[k][i, r, :, chans : 2 * chans].astype(F32)

    def doubled(k, i, phase, r):
        pair = big[k + 1][i, pl.ds(r, 2), :, chans : 2 * chans]
        return mm(ups[k][phase], pair.reshape(cols[k], chans))

    for i in range(images):
        for y in range(rows[3]):
            put(3, i, y + 1, lats[3][i, y])
    halo_wait(3)
    for i in range(images):
        put(3, i, 0, jnp.where(first, center(3, i, 1), recvs[3][0, i].astype(F32)))
        put(3, i, rows[3] + 1, jnp.where(last, center(3, i, rows[3]), recvs[3][1, i].astype(F32)))

    def clear(k):
        @pl.when(first)
        def _():
            for i in range(images):
                big[k][i, 0] = jnp.zeros_like(big[k][i, 0])

        @pl.when(last)
        def _():
            for i in range(images):
                big[k][i, rows[k] + 1] = jnp.zeros_like(big[k][i, rows[k] + 1])

    def edges(k):
        for i in range(images):
            above = recvs[k][0, i].astype(F32) + doubled(k, i, 1, 0)
            below = recvs[k][1, i].astype(F32) + doubled(k, i, 0, rows[k] // 2)
            put(k, i, 0, jnp.where(first, center(k, i, 1), above))
            put(k, i, rows[k] + 1, jnp.where(last, center(k, i, rows[k]), below))

    for k in (2, 1):
        for i in range(images):
            for j in range(rows[k] // 2):
                put(k, i, 2 * j + 1, lats[k][i, 2 * j] + doubled(k, i, 0, j))
                put(k, i, 2 * j + 2, lats[k][i, 2 * j + 1] + doubled(k, i, 1, j + 1))
        halo_wait(k)
        edges(k)
        clear(k + 1)

    pairs = rows[0] // 2

    def merge_two(t, carry):
        i, j = t // pairs, t % pairs
        both = mm(feat[0][i, pl.ds(2 * j, 2)].reshape(2 * cols[0], -1), lat_w[0][...])
        both = both + bias[0:1, :]
        put(0, i, 2 * j + 1, both[: cols[0]] + doubled(0, i, 0, j))
        put(0, i, 2 * j + 2, both[cols[0] :] + doubled(0, i, 1, j + 1))
        return carry

    lax.fori_loop(0, images * pairs, merge_two, 0)

    def conv_rows(k, i, y, count):
        total = None
        for a in range(3):
            band = big[k][i, pl.ds(y + a, count)].reshape(count * cols[k], 3 * chans)
            part = mm(band, smooth[k, a])
            total = part if total is None else total + part
        conv[k][i, pl.ds(y, count)] = total.reshape(count, cols[k], chans)
        return jnp.sum(total, 0, keepdims=True), jnp.sum(total * total, 0, keepdims=True)

    stat_rest[...] = jnp.zeros_like(stat_rest)
    stat_two[...] = jnp.zeros_like(stat_two)

    def conv_whole(k):
        smooth_copy[k].wait()
        for i in range(images):
            total, square = conv_rows(k, i, 0, rows[k])
            slot = ((k - 1) * images + i) * 2
            stat_rest[slot : slot + 1, :] = total
            stat_rest[slot + 1 : slot + 2, :] = square

    conv_whole(3)
    conv_whole(2)

    smooth_copy[0].wait()
    inner = (rows[0] - 2) // 2
    for i in range(images):

        def conv_two(t, carry):
            total, square = conv_rows(0, i, 1 + 2 * t, 2)
            return carry[0] + total, carry[1] + square

        zero = jnp.zeros((1, chans), F32)
        total, square = lax.fori_loop(0, inner, conv_two, (zero, zero))
        stat_two[2 * i : 2 * i + 1, :] = total
        stat_two[2 * i + 1 : 2 * i + 2, :] = square
    halo_wait(0)
    edges(0)
    clear(0)
    clear(1)

    def conv_edges(t, carry):
        i, y = t // 2, (t % 2) * (rows[0] - 1)
        total, square = conv_rows(0, i, y, 1)
        stat_two[pl.ds(2 * i, 1), :] += total
        stat_two[pl.ds(2 * i + 1, 1), :] += square
        return carry

    lax.fori_loop(0, images * 2, conv_edges, 0)

    def stat_copies(mine, got, send_sem, recv_sem):
        return [
            pltpu.make_async_remote_copy(
                src_ref=mine,
                dst_ref=got.at[d],
                send_sem=send_sem.at[d],
                recv_sem=recv_sem.at[d],
                device_id={"rows": lax.rem(me + d, n)},
                device_id_type=MESH,
            )
            for d in range(1, n)
        ]

    two_copies = stat_copies(stat_two, got_two, two_send, two_recv)
    for copy in two_copies:
        copy.start()
    conv_whole(1)
    rest_copies = stat_copies(stat_rest, got_rest, rest_send, rest_recv)
    for copy in rest_copies:
        copy.start()

    size = chans // GROUPS
    same = lax.broadcasted_iota(jnp.int32, (chans, chans), 0) // size
    same = same == lax.broadcasted_iota(jnp.int32, (chans, chans), 1) // size
    same = jnp.where(same, 1.0, 0.0).astype(F32)

    def gathered(mine, got):
        total = mine[...]
        for d in range(1, n):
            total = total + got[d]
        return jnp.dot(
            total, same, precision=lax.Precision.HIGHEST, preferred_element_type=F32
        )

    for copy in two_copies:
        copy.wait_recv()
    sums_two[...] = gathered(stat_two, got_two)
    for copy in rest_copies:
        copy.wait_recv()
    sums_rest[...] = gathered(stat_rest, got_rest)
    for k in range(4):
        sent_wait(k)
    for copy in two_copies + rest_copies:
        copy.wait_send()


def finish_kernel(n, geom, *refs):
    images, chans = geom["images"], geom["chans"]
    rows, cols = geom["rows"], geom["cols"]
    conv, (sums_two, sums_rest, gain, shift) = refs[0:4], refs[4:8]
    out_hbm, staged, out_sem = refs[8:12], refs[12:16], refs[16]
    size = chans // GROUPS

    def finish(k, i, total, square):
        entries = float(rows[k] * n * cols[k] * size)
        mean = total / entries
        variance = square / entries - mean * mean
        scale = lax.rsqrt(variance + EPSILON) * gain[k : k + 1, :]
        offset = shift[k : k + 1, :]

        def row(y, carry):
            staged[k][i, y] = ((conv[k][i, y] - mean) * scale + offset).astype(BF16)
            return carry

        lax.fori_loop(0, rows[k], row, 0)
        copy = pltpu.make_async_copy(staged[k].at[i], out_hbm[k].at[i], out_sem.at[k, i])
        copy.start()
        return copy

    out_copies = []
    for k in range(4):
        for i in range(images):
            sums = sums_rest if k else sums_two
            slot = (max(k - 1, 0) * images + i) * 2
            out_copies.append(
                finish(k, i, sums[slot : slot + 1, :], sums[slot + 1 : slot + 2, :])
            )
    for copy in out_copies:
        copy.wait()


def per_device(n, *args):
    feats, lat_ws = args[0:4], args[4:8]
    bias, smooth, gain, shift = args[8:12]
    images, chans = feats[0].shape[0], lat_ws[0].shape[1]
    rows = [f.shape[1] for f in feats]
    cols = [f.shape[2] for f in feats]
    geom = {"images": images, "chans": chans, "rows": rows, "cols": cols}
    any_spec = pl.BlockSpec(memory_space=pltpu.HBM)
    vmem_spec = pl.BlockSpec(memory_space=pltpu.VMEM)
    outs = [jax.ShapeDtypeStruct((images, r, c, chans), BF16) for r, c in zip(rows, cols)]
    dma = pltpu.SemaphoreType.DMA
    rest_rows = -(-(3 * images * 2) // 8) * 8
    two_rows = -(-(images * 2) // 8) * 8
    scratch = (
        [pltpu.VMEM(f.shape, BF16) for f in feats]
        + [pltpu.VMEM(w.shape, BF16) for w in lat_ws]
        + [pltpu.VMEM(smooth.shape, BF16)]
        + [pltpu.VMEM((images, r + 2, c, 3 * chans), BF16) for r, c in zip(rows, cols)]
        + [pltpu.VMEM((2, images, c, chans), BF16) for c in cols]
        + [pltpu.VMEM((2, images, c, chans), BF16) for c in cols]
        + [pltpu.VMEM(o.shape, F32) for o in outs[1:]]
        + [pltpu.VMEM((2, c, c), BF16) for c in cols[:3]]
        + [
            pltpu.VMEM((two_rows, chans), F32),
            pltpu.VMEM((rest_rows, chans), F32),
            pltpu.VMEM((n, two_rows, chans), F32),
            pltpu.VMEM((n, rest_rows, chans), F32),
        ]
        + [dma((4,)), dma((4,)), dma((4,))]
        + [dma((4, 2)), dma((4, 2)), dma((n,)), dma((n,)), dma((n,)), dma((n,))]
    )
    held = pl.pallas_call(
        functools.partial(kernel, n, geom),
        out_shape=[pltpu.VMEM(o.shape, F32) for o in outs]
        + [pltpu.VMEM((two_rows, chans), F32), pltpu.VMEM((rest_rows, chans), F32)],
        in_specs=[any_spec] * 8 + [vmem_spec, any_spec],
        out_specs=[vmem_spec] * 6,
        scratch_shapes=scratch,
        compiler_params=pltpu.CompilerParams(
            collective_id=0, has_side_effects=True, vmem_limit_bytes=KERNEL_BYTES
        ),
    )(*args[:10])
    held = [pltpu.with_memory_space_constraint(h, pltpu.VMEM) for h in held]
    return pl.pallas_call(
        functools.partial(finish_kernel, n, geom),
        out_shape=outs,
        in_specs=[vmem_spec] * 8,
        out_specs=[any_spec] * 4,
        scratch_shapes=[pltpu.VMEM(o.shape, BF16) for o in outs] + [dma((4, images))],
        compiler_params=pltpu.CompilerParams(vmem_limit_bytes=16 * 1024 * 1024),
    )(*held, gain, shift)


def solution(mesh):
    strips = P("batch", "rows", None, None)
    run = functools.partial(per_device, mesh.shape["rows"])
    return jax.shard_map(
        lambda *args: tuple(run(*args)),
        mesh=mesh,
        in_specs=(strips,) * 4 + (P(),) * 8,
        out_specs=(strips,) * 4,
        check_vma=False,
    )
```

```python
import functools

import jax
import jax.numpy as jnp
from jax import lax
from jax.experimental import pallas as pl
from jax.experimental.pallas import tpu as pltpu
from jax.sharding import PartitionSpec as P

GROUPS = 32
EPSILON = 1e-05
F32 = jnp.float32
BF16 = jnp.bfloat16
MESH = pl.DeviceIdType.MESH
KERNEL_BYTES = 56 * 1024 * 1024


def bilinear(cols):
    half = cols // 2
    fine = lax.broadcasted_iota(jnp.int32, (cols, cols), 0)
    coarse = lax.broadcasted_iota(jnp.int32, (cols, cols), 1)
    second = coarse >= half
    coarse = jnp.where(second, coarse - half, coarse)
    near = fine // 2
    odd = fine % 2 == 1
    far = jnp.where(odd, jnp.minimum(near + 1, half - 1), jnp.maximum(near - 1, 0))
    value = jnp.where(coarse == near, 0.75, 0.0) + jnp.where(coarse == far, 0.25, 0.0)
    even_rows = value * jnp.where(second, 0.75, 0.25)
    odd_rows = value * jnp.where(second, 0.25, 0.75)
    return even_rows.astype(BF16), odd_rows.astype(BF16)


def mm(a, b):
    return jnp.dot(a, b, preferred_element_type=F32)


def kernel(n, geom, *refs):
    images, chans = geom["images"], geom["chans"]
    rows, cols = geom["rows"], geom["cols"]
    it = iter(refs)
    take = lambda count: [next(it) for _ in range(count)]
    feat_hbm, lat_hbm = take(4), take(4)
    bias, smooth_hbm = take(2)
    conv = take(4)
    sums_two, sums_rest = take(2)
    feat, lat_w = take(4), take(4)
    (smooth,) = take(1)
    big, sends, recvs = take(4), take(4), take(4)
    lats = [None] + take(3)
    ups = take(3)
    stat_two, stat_rest, got_two, got_rest = take(4)
    in_sem, w_sem, s_sem = take(3)
    halo_send, halo_recv, two_send, two_recv, rest_send, rest_recv = take(6)

    me = lax.axis_index("rows")
    first, last = me == 0, me == n - 1

    feat_copy = [pltpu.make_async_copy(feat_hbm[k], feat[k], in_sem.at[k]) for k in range(4)]
    lat_copy = [pltpu.make_async_copy(lat_hbm[k], lat_w[k], w_sem.at[k]) for k in range(4)]
    smooth_copy = [
        pltpu.make_async_copy(smooth_hbm.at[k], smooth.at[k], s_sem.at[k]) for k in range(4)
    ]
    for k in (3, 2, 1, 0):
        lat_copy[k].start()
        feat_copy[k].start()
    for k in (3, 2, 0, 1):
        smooth_copy[k].start()

    barrier = pltpu.get_barrier_semaphore()
    for d in range(1, n):
        pl.semaphore_signal(
            barrier, inc=1, device_id={"rows": lax.rem(me + d, n)}, device_id_type=MESH
        )

    @pl.when(first)
    def _():
        for k in range(4):
            recvs[k][0] = jnp.zeros_like(recvs[k][0])

    @pl.when(last)
    def _():
        for k in range(4):
            recvs[k][1] = jnp.zeros_like(recvs[k][1])

    for k in range(3):
        even, odd = bilinear(cols[k])
        ups[k][0] = even
        ups[k][1] = odd

    def halo_copy(k, way):
        return pltpu.make_async_remote_copy(
            src_ref=sends[k].at[way],
            dst_ref=recvs[k].at[1 - way],
            send_sem=halo_send.at[k, way],
            recv_sem=halo_recv.at[k, 1 - way],
            device_id={"rows": lax.rem(me + (1 if way else n - 1), n)},
            device_id_type=MESH,
        )

    def halo_start(k):
        @pl.when(jnp.logical_not(first))
        def _():
            halo_copy(k, 0).start()

        @pl.when(jnp.logical_not(last))
        def _():
            halo_copy(k, 1).start()

    def halo_wait(k):
        @pl.when(jnp.logical_not(last))
        def _():
            halo_copy(k, 0).wait_recv()

        @pl.when(jnp.logical_not(first))
        def _():
            halo_copy(k, 1).wait_recv()

    def sent_wait(k):
        @pl.when(jnp.logical_not(first))
        def _():
            halo_copy(k, 0).wait_send()

        @pl.when(jnp.logical_not(last))
        def _():
            halo_copy(k, 1).wait_send()

    for k in (3, 2, 1):
        lat_copy[k].wait()
        feat_copy[k].wait()
        for i in range(images):
            flat = feat[k][i].reshape(rows[k] * cols[k], feat[k].shape[-1])
            value = mm(flat, lat_w[k][...]) + bias[k : k + 1, :]
            lats[k][i] = value.reshape(rows[k], cols[k], chans)
            sends[k][0, i] = value[: cols[k]].astype(BF16)
            sends[k][1, i] = value[(rows[k] - 1) * cols[k] :].astype(BF16)
        if k == 3:
            pl.semaphore_wait(barrier, n - 1)
        halo_start(k)
    lat_copy[0].wait()
    feat_copy[0].wait()
    for i in range(images):
        for way, y in ((0, 0), (1, rows[0] - 1)):
            sends[0][way, i] = (mm(feat[0][i, y], lat_w[0][...]) + bias[0:1, :]).astype(BF16)
    halo_start(0)

    def put(k, i, r, value):
        width = cols[k]
        spot = lax.broadcasted_iota(jnp.int32, value.shape, 0)
        before = jnp.where(spot == 0, 0.0, pltpu.roll(value, 1, 0))
        beyond = jnp.where(spot == width - 1, 0.0, pltpu.roll(value, width - 1, 0))
        big[k][i, r, :, 0:chans] = before.astype(BF16)
        big[k][i, r, :, chans : 2 * chans] = value.astype(BF16)
        big[k][i, r, :, 2 * chans :] = beyond.astype(BF16)

    def center(k, i, r):
        return big[k][i, r, :, chans : 2 * chans].astype(F32)

    def doubled(k, i, phase, r):
        pair = big[k + 1][i, pl.ds(r, 2), :, chans : 2 * chans]
        return mm(ups[k][phase], pair.reshape(cols[k], chans))

    for i in range(images):
        for y in range(rows[3]):
            put(3, i, y + 1, lats[3][i, y])
    halo_wait(3)
    for i in range(images):
        put(3, i, 0, jnp.where(first, center(3, i, 1), recvs[3][0, i].astype(F32)))
        put(3, i, rows[3] + 1, jnp.where(last, center(3, i, rows[3]), recvs[3][1, i].astype(F32)))

    def clear(k):
        @pl.when(first)
        def _():
            for i in range(images):
                big[k][i, 0] = jnp.zeros_like(big[k][i, 0])

        @pl.when(last)
        def _():
            for i in range(images):
                big[k][i, rows[k] + 1] = jnp.zeros_like(big[k][i, rows[k] + 1])

    def edges(k):
        for i in range(images):
            above = recvs[k][0, i].astype(F32) + doubled(k, i, 1, 0)
            below = recvs[k][1, i].astype(F32) + doubled(k, i, 0, rows[k] // 2)
            put(k, i, 0, jnp.where(first, center(k, i, 1), above))
            put(k, i, rows[k] + 1, jnp.where(last, center(k, i, rows[k]), below))

    def conv_rows(k, i, y, count):
        total = None
        for a in range(3):
            band = big[k][i, pl.ds(y + a, count)].reshape(count * cols[k], 3 * chans)
            part = mm(band, smooth[k, a])
            total = part if total is None else total + part
        conv[k][i, pl.ds(y, count)] = total.reshape(count, cols[k], chans)
        return jnp.sum(total, 0, keepdims=True), jnp.sum(total * total, 0, keepdims=True)

    stat_rest[...] = jnp.zeros_like(stat_rest)
    stat_two[...] = jnp.zeros_like(stat_two)

    def conv_whole(k):
        smooth_copy[k].wait()
        for i in range(images):
            total, square = conv_rows(k, i, 0, rows[k])
            slot = ((k - 1) * images + i) * 2
            stat_rest[slot : slot + 1, :] = total
            stat_rest[slot + 1 : slot + 2, :] = square

    for k in (2, 1):
        for i in range(images):
            for j in range(rows[k] // 2):
                put(k, i, 2 * j + 1, lats[k][i, 2 * j] + doubled(k, i, 0, j))
                put(k, i, 2 * j + 2, lats[k][i, 2 * j + 1] + doubled(k, i, 1, j + 1))
        if k == 1:
            conv_whole(3)
        halo_wait(k)
        edges(k)
        clear(k + 1)

    pairs = rows[0] // 2

    def merge_two(t, carry):
        i, j = t // pairs, t % pairs
        both = mm(feat[0][i, pl.ds(2 * j, 2)].reshape(2 * cols[0], -1), lat_w[0][...])
        both = both + bias[0:1, :]
        put(0, i, 2 * j + 1, both[: cols[0]] + doubled(0, i, 0, j))
        put(0, i, 2 * j + 2, both[cols[0] :] + doubled(0, i, 1, j + 1))
        return carry

    lax.fori_loop(0, images * pairs, merge_two, 0)

    clear(1)
    conv_whole(2)

    def stat_copies(mine, got, send_sem, recv_sem):
        return [
            pltpu.make_async_remote_copy(
                src_ref=mine,
                dst_ref=got.at[d],
                send_sem=send_sem.at[d],
                recv_sem=recv_sem.at[d],
                device_id={"rows": lax.rem(me + d, n)},
                device_id_type=MESH,
            )
            for d in range(1, n)
        ]

    smooth_copy[0].wait()
    inner = (rows[0] - 2) // 2
    for i in range(images):

        def conv_two(t, carry):
            total, square = conv_rows(0, i, 1 + 2 * t, 2)
            return carry[0] + total, carry[1] + square

        zero = jnp.zeros((1, chans), F32)
        total, square = lax.fori_loop(0, inner, conv_two, (zero, zero))
        stat_two[2 * i : 2 * i + 1, :] = total
        stat_two[2 * i + 1 : 2 * i + 2, :] = square
    conv_whole(1)
    rest_copies = stat_copies(stat_rest, got_rest, rest_send, rest_recv)
    for copy in rest_copies:
        copy.start()
    halo_wait(0)
    edges(0)
    clear(0)

    def conv_edges(t, carry):
        i, y = t // 2, (t % 2) * (rows[0] - 1)
        total, square = conv_rows(0, i, y, 1)
        stat_two[pl.ds(2 * i, 1), :] += total
        stat_two[pl.ds(2 * i + 1, 1), :] += square
        return carry

    lax.fori_loop(0, images * 2, conv_edges, 0)

    two_copies = stat_copies(stat_two, got_two, two_send, two_recv)
    for copy in two_copies:
        copy.start()

    size = chans // GROUPS
    same = lax.broadcasted_iota(jnp.int32, (chans, chans), 0) // size
    same = same == lax.broadcasted_iota(jnp.int32, (chans, chans), 1) // size
    same = jnp.where(same, 1.0, 0.0).astype(F32)

    def gathered(mine, got):
        total = mine[...]
        for d in range(1, n):
            total = total + got[d]
        return jnp.dot(
            total, same, precision=lax.Precision.HIGHEST, preferred_element_type=F32
        )

    for copy in rest_copies:
        copy.wait_recv()
    sums_rest[...] = gathered(stat_rest, got_rest)
    for copy in two_copies:
        copy.wait_recv()
    sums_two[...] = gathered(stat_two, got_two)
    for k in range(4):
        sent_wait(k)
    for copy in two_copies + rest_copies:
        copy.wait_send()


def finish_kernel(n, geom, *refs):
    images, chans = geom["images"], geom["chans"]
    rows, cols = geom["rows"], geom["cols"]
    conv, (sums_two, sums_rest, gain, shift) = refs[0:4], refs[4:8]
    out_hbm, staged, out_sem = refs[8:12], refs[12:16], refs[16]
    size = chans // GROUPS

    def finish(k, i, total, square):
        entries = float(rows[k] * n * cols[k] * size)
        mean = total / entries
        variance = square / entries - mean * mean
        scale = lax.rsqrt(variance + EPSILON) * gain[k : k + 1, :]
        offset = shift[k : k + 1, :]

        def row(y, carry):
            staged[k][i, y] = ((conv[k][i, y] - mean) * scale + offset).astype(BF16)
            return carry

        lax.fori_loop(0, rows[k], row, 0)
        copy = pltpu.make_async_copy(staged[k].at[i], out_hbm[k].at[i], out_sem.at[k, i])
        copy.start()
        return copy

    out_copies = []
    for k in range(4):
        for i in range(images):
            sums = sums_rest if k else sums_two
            slot = (max(k - 1, 0) * images + i) * 2
            out_copies.append(
                finish(k, i, sums[slot : slot + 1, :], sums[slot + 1 : slot + 2, :])
            )
    for copy in out_copies:
        copy.wait()


def per_device(n, *args):
    feats, lat_ws = args[0:4], args[4:8]
    bias, smooth, gain, shift = args[8:12]
    images, chans = feats[0].shape[0], lat_ws[0].shape[1]
    rows = [f.shape[1] for f in feats]
    cols = [f.shape[2] for f in feats]
    geom = {"images": images, "chans": chans, "rows": rows, "cols": cols}
    any_spec = pl.BlockSpec(memory_space=pltpu.HBM)
    vmem_spec = pl.BlockSpec(memory_space=pltpu.VMEM)
    outs = [jax.ShapeDtypeStruct((images, r, c, chans), BF16) for r, c in zip(rows, cols)]
    dma = pltpu.SemaphoreType.DMA
    rest_rows = -(-(3 * images * 2) // 8) * 8
    two_rows = -(-(images * 2) // 8) * 8
    scratch = (
        [pltpu.VMEM(f.shape, BF16) for f in feats]
        + [pltpu.VMEM(w.shape, BF16) for w in lat_ws]
        + [pltpu.VMEM(smooth.shape, BF16)]
        + [pltpu.VMEM((images, r + 2, c, 3 * chans), BF16) for r, c in zip(rows, cols)]
        + [pltpu.VMEM((2, images, c, chans), BF16) for c in cols]
        + [pltpu.VMEM((2, images, c, chans), BF16) for c in cols]
        + [pltpu.VMEM(o.shape, F32) for o in outs[1:]]
        + [pltpu.VMEM((2, c, c), BF16) for c in cols[:3]]
        + [
            pltpu.VMEM((two_rows, chans), F32),
            pltpu.VMEM((rest_rows, chans), F32),
            pltpu.VMEM((n, two_rows, chans), F32),
            pltpu.VMEM((n, rest_rows, chans), F32),
        ]
        + [dma((4,)), dma((4,)), dma((4,))]
        + [dma((4, 2)), dma((4, 2)), dma((n,)), dma((n,)), dma((n,)), dma((n,))]
    )
    held = pl.pallas_call(
        functools.partial(kernel, n, geom),
        out_shape=[pltpu.VMEM(o.shape, F32) for o in outs]
        + [pltpu.VMEM((two_rows, chans), F32), pltpu.VMEM((rest_rows, chans), F32)],
        in_specs=[any_spec] * 8 + [vmem_spec, any_spec],
        out_specs=[vmem_spec] * 6,
        scratch_shapes=scratch,
        compiler_params=pltpu.CompilerParams(
            collective_id=0, has_side_effects=True, vmem_limit_bytes=KERNEL_BYTES
        ),
    )(*args[:10])
    held = [pltpu.with_memory_space_constraint(h, pltpu.VMEM) for h in held]
    return pl.pallas_call(
        functools.partial(finish_kernel, n, geom),
        out_shape=outs,
        in_specs=[vmem_spec] * 8,
        out_specs=[any_spec] * 4,
        scratch_shapes=[pltpu.VMEM(o.shape, BF16) for o in outs] + [dma((4, images))],
        compiler_params=pltpu.CompilerParams(vmem_limit_bytes=16 * 1024 * 1024),
    )(*held, gain, shift)


def solution(mesh):
    strips = P("batch", "rows", None, None)
    run = functools.partial(per_device, mesh.shape["rows"])
    return jax.shard_map(
        lambda *args: tuple(run(*args)),
        mesh=mesh,
        in_specs=(strips,) * 4 + (P(),) * 8,
        out_specs=(strips,) * 4,
        check_vma=False,
    )
```
